32 devices in a mesh: dp: 16 (over z, y, x), mp: 2 (over core).
Axes of the slice: x: 2, y: 2, z: 4, core: 2. Of those that a mesh axis runs over, the one named last changes fastest.
Arguments:
- clean_latent: float32 [16, 4096], P('dp'), may hold values from -6 to 6
- noise_draw: float32 [16, 4096], P('dp'), may hold values from -6 to 6
- timestep: int32 [16], P('dp'), may hold values from 1 to 8
- bucket: int32 [16], P('dp'), may hold values from 0 to 7
- bucket_weights: float32 [8], replicated, may hold values from 0.25 to 4
- teacher_embed: float32 [16, 2048], replicated, may hold values from -1.5 to 1.5
- teacher_final: float32 [16, 2048], replicated, may hold values from -0.125 to 0.125
- teacher_mod: float32 [16, 3, 2048], replicated, may hold values from -3 to 3
- teacher_qkv: bfloat16 [2048, 3, 1024], P(None, None, 'mp'), may hold values from -1 to 1
- teacher_out: bfloat16 [2048, 1024], P(None, 'mp'), may hold values from -0.1875 to 0.1875
- student_embed: float32 [16, 2048], replicated, may hold values from -1.5 to 1.5
- student_final: float32 [16, 2048], replicated, may hold values from -0.125 to 0.125
- student_mod: float32 [8, 3, 2048], replicated, may hold values from -3 to 3
- student_qkv: bfloat16 [2048, 3, 1024], P('dp', None, 'mp'), may hold values from -1 to 1
- student_out: bfloat16 [2048, 1024], P('dp', 'mp'), may hold values from -0.1875 to 0.1875
- moment_qkv: float32 [2048, 3, 1024], P('dp', None, 'mp'), may hold values from -2 to 2
- second_qkv: float32 [2048, 3, 1024], P('dp', None, 'mp'), may hold values from 0.05 to 0.5
- moment_out: float32 [2048, 1024], P('dp', 'mp'), may hold values from -2 to 2
- second_out: float32 [2048, 1024], P('dp', 'mp'), may hold values from 0.05 to 0.5
Outputs:
- new_moment_qkv: float32 [2048, 3, 1024], P('dp', None, 'mp')
- new_second_qkv: float32 [2048, 3, 1024], P('dp', None, 'mp')
- update_qkv: float32 [2048, 3, 1024], P('dp', None, 'mp')
- new_moment_out: float32 [2048, 1024], P('dp', 'mp')
- new_second_out: float32 [2048, 1024], P('dp', 'mp')
- update_out: float32 [2048, 1024], P('dp', 'mp')
- loss: float32 [], replicated
The draws below stay inside these ranges and needn't reach their ends.
All inputs are finite; a program needn't handle non-finite values.
Results may differ from the reference program's by a relative error of at most 0.00035.
Values may be sent and summed in bfloat16 or wider, within the bound.
No kernel may reach another device: no remote copies, remote signals or barrier semaphores. Data moves between devices by JAX's collectives and lax.ppermute only.
A program may use at most 128 MiB of HBM per device.

```python
import math
import jax
import jax.numpy as jnp
from jax import lax

D = 2048
HEADS = 16
HS = 64
INNER = 1024
PATCH_CH = 16
SEQ = 256
LATENT = 4096
SAMPLES = 16
K = 8
TGRID = 16
NBUCKET = 8


def aligned_projection(seed_key, salt):
    folded = jax.random.fold_in(seed_key, salt)
    initial = jax.random.normal(folded, (D, 3, INNER), jnp.float32) / math.sqrt(D)
    return jnp.clip(initial, -1.0, 1.0).astype(jnp.bfloat16)


def draw_teacher_qkv(key, part):
    return aligned_projection(key, 11)


def draw_student_qkv(key, part):
    return aligned_projection(key, 23)


def set_ends(entries, key, smallest, largest):
    place = [jax.random.randint(jax.random.fold_in(key, axis), (), 0, length) for axis, length in enumerate(entries.shape)]
    longest = entries.shape.index(max(entries.shape))
    next_to = place[:longest] + [(place[longest] + 1) % entries.shape[longest]] + place[longest + 1:]
    return entries.at[tuple(place)].set(smallest).at[tuple(next_to)].set(largest)


def block_scale(key, extent, shards, least, high):
    gain = 1.0
    for position, blocks in shards:
        draws = jax.random.uniform(jax.random.fold_in(jax.random.fold_in(key, 6), position), (blocks,), jnp.float32, least / len(shards), high / len(shards))
        gain = gain * jnp.repeat(jnp.exp(draws), extent[position] // blocks).reshape((-1,) + (1,) * (len(extent) - 1 - position))
    return gain


def noise(rng, extent, scale, bound, shards=(), kind=jnp.bfloat16):
    values = jax.random.normal(rng, extent, jnp.float32) * scale
    if len(shards) > 0:
        values = block_scale(rng, extent, shards, -0.22, 0.18) * values
    return jnp.clip(values, min=-bound, max=bound).astype(kind)


def setup_inputs(seed: int = 0) -> dict:
    splits = jax.random.split(jax.random.key(seed), 20)
    return {
        "clean_latent": noise(splits[0], (SAMPLES, LATENT), 1.0, 6.0, ((0, 16),), jnp.float32),
        "noise_draw": noise(splits[1], (SAMPLES, LATENT), 1.0, 6.0, ((0, 16),), jnp.float32),
        "timestep": set_ends(jax.random.randint(splits[2], (SAMPLES,), 1, K + 1), jax.random.fold_in(splits[2], 1), 1, K).astype(jnp.int32),
        "bucket": set_ends(jax.random.randint(splits[3], (SAMPLES,), 0, NBUCKET), jax.random.fold_in(splits[3], 1), 0, NBUCKET - 1).astype(jnp.int32),
        "bucket_weights": jnp.clip(jnp.exp(jax.random.uniform(splits[4], (NBUCKET,), jnp.float32, math.log(0.25), math.log(4.0))), 0.25, 4.0),
        "teacher_embed": noise(splits[5], (PATCH_CH, D), PATCH_CH ** -0.5, 1.5, (), jnp.float32),
        "teacher_final": noise(splits[6], (PATCH_CH, D), D ** -0.5, 0.125, (), jnp.float32),
        "teacher_mod": noise(splits[7], (TGRID, 3, D), 0.5, 3.0, (), jnp.float32),
        "teacher_qkv": draw_teacher_qkv(jax.random.fold_in(splits[19], 71), 0),
        "teacher_out": noise(splits[9], (D, INNER), INNER ** -0.5, 0.1875, ((1, 2),)),
        "student_embed": noise(splits[10], (PATCH_CH, D), PATCH_CH ** -0.5, 1.5, (), jnp.float32),
        "student_final": noise(splits[11], (PATCH_CH, D), D ** -0.5, 0.125, (), jnp.float32),
        "student_mod": noise(splits[12], (K, 3, D), 0.5, 3.0, (), jnp.float32),
        "student_qkv": draw_student_qkv(jax.random.fold_in(splits[19], 71), 0),
        "student_out": noise(splits[14], (D, INNER), INNER ** -0.5, 0.1875, ((0, 16), (1, 2))),
        "moment_qkv": noise(splits[15], (D, 3, INNER), 0.3, 2.0, ((0, 16), (2, 2)), jnp.float32),
        "second_qkv": jnp.clip(jnp.exp(math.log(0.5) - 2.3025851 * jax.random.uniform(splits[16], (D, 3, INNER), jnp.float32) ** block_scale(splits[16], (D, 3, INNER), ((0, 16), (2, 2)), -0.2, 0.2)), 0.05, 0.5),
        "moment_out": noise(splits[17], (D, INNER), 0.3, 2.0, ((0, 16), (1, 2)), jnp.float32),
        "second_out": jnp.clip(jnp.exp(math.log(0.5) - 2.3025851 * jax.random.uniform(splits[18], (D, INNER), jnp.float32) ** block_scale(splits[18], (D, INNER), ((0, 16), (1, 2)), -0.2, 0.2)), 0.05, 0.5),
    }


LN_EPS = 0.01
BETA_ONE = 0.9
BETA_TWO = 0.99
ADAM_EPS = 1e-08

def plan():
    grid = jnp.arange(TGRID + 1, dtype=jnp.float32)
    lamb = 6.0 - 12.0 * grid / TGRID
    return (jnp.sqrt(jax.nn.sigmoid(lamb)), jnp.sqrt(jax.nn.sigmoid(-lamb)))

def positions():
    index = jnp.arange(SEQ, dtype=jnp.float32)[:, None]
    half = D // 2
    freqs = jnp.exp(-math.log(10000.0) * jnp.arange(half, dtype=jnp.float32) / half)
    angles = index * freqs[None, :]
    return jnp.concatenate([jnp.sin(angles), jnp.cos(angles)], axis=1)

def normalize(values):
    center = values - lax.optimization_barrier(jnp.mean(values, axis=-1, keepdims=True))
    inverse = lax.rsqrt(lax.optimization_barrier(jnp.mean(center * center, axis=-1, keepdims=True)) + LN_EPS)
    return (center * inverse, inverse)

def norm_back(upstream, normed, inverse):
    first_mean = lax.optimization_barrier(jnp.mean(upstream, axis=-1, keepdims=True))
    second_mean = lax.optimization_barrier(jnp.mean(upstream * normed, axis=-1, keepdims=True))
    return (upstream - first_mean - normed * second_mean) * inverse

def front(latent, modrow, embed, w_qkv, w_out, placed):
    hidden = jnp.dot(latent, embed, precision=lax.Precision.HIGHEST) + placed
    normed, unused = normalize(hidden)
    shaped = (normed * (1.0 + modrow[1]) + modrow[0]).astype(jnp.bfloat16)
    packed = jnp.dot(shaped, w_qkv.reshape(D, 3 * INNER), preferred_element_type=jnp.float32)
    packed = packed.astype(jnp.bfloat16).reshape(SEQ, 3, HEADS, HS)
    queries = packed[:, 0]
    keys_all = packed[:, 1]
    values = packed[:, 2]
    scores = jnp.einsum('qhd,khd->hqk', queries.astype(jnp.float32), keys_all.astype(jnp.float32)) / math.sqrt(HS)
    weights = jax.nn.softmax(scores, axis=-1)
    rounded = weights.astype(jnp.bfloat16)
    attended = jnp.einsum('hqk,khd->qhd', rounded.astype(jnp.float32), values.astype(jnp.float32))
    attended = attended.astype(jnp.bfloat16).reshape(SEQ, INNER)
    projected = lax.dot_general(attended, w_out, (((1,), (1,)), ((), ())), preferred_element_type=jnp.float32)
    return (hidden, shaped, queries, keys_all, values, weights, rounded, attended, projected)

def tail(hidden, modrow, projected, final):
    mixed = hidden + modrow[2] * projected
    normed, inverse = normalize(mixed)
    predicted = jnp.dot(normed, final.T, precision=lax.Precision.HIGHEST)
    return (predicted, normed, inverse)

def reference(clean_latent, noise_draw, timestep, bucket, bucket_weights, teacher_embed, teacher_final, teacher_mod, teacher_qkv, teacher_out, student_embed, student_final, student_mod, student_qkv, student_out, moment_qkv, second_qkv, moment_out, second_out):
    alphas, sigmas = plan()
    placed = positions()

    def teacher_eps(latent, modrow):
        parts = front(latent, modrow, teacher_embed, teacher_qkv, teacher_out, placed)
        return tail(parts[0], modrow, parts[8], teacher_final)[0]

    def sample_step(carry, inputs):
        clean_row, noise_row, step_index, bucket_id = inputs
        first = 2 * step_index
        middle = first - 1
        last = first - 2
        a_first, s_first = (alphas[first], sigmas[first])
        a_middle, s_middle = (alphas[middle], sigmas[middle])
        a_last, s_last = (alphas[last], sigmas[last])
        latent0 = (a_first * clean_row + s_first * noise_row).reshape(SEQ, PATCH_CH)
        eps_zero = teacher_eps(latent0, teacher_mod[first - 1])
        latent1 = a_middle * (latent0 - s_first * eps_zero) / a_first + s_middle * eps_zero
        eps_one = teacher_eps(latent1, teacher_mod[middle - 1])
        latent2 = a_last * (latent1 - s_middle * eps_one) / a_middle + s_last * eps_one
        target = (latent0 - a_first / a_last * latent2) / (s_first - a_first * s_last / a_last)
        modrow = student_mod[step_index - 1]
        hidden, shaped, queries, keys_all, values, weights, rounded, attended, projected = front(latent0, modrow, student_embed, student_qkv, student_out, placed)
        predicted, normed, inverse = tail(hidden, modrow, projected, student_final)
        weight = bucket_weights[bucket_id]
        error = predicted - target
        sample_loss = weight * jnp.sum(error * error)
        d_pred = 2.0 * weight * error
        d_normed = jnp.dot(d_pred, student_final, precision=lax.Precision.HIGHEST)
        d_mixed = norm_back(d_normed, normed, inverse)
        d_proj = (modrow[2] * d_mixed).astype(jnp.bfloat16)
        grad_out = lax.dot_general(d_proj, attended, (((0,), (0,)), ((), ())), preferred_element_type=jnp.float32)
        d_attn = jnp.dot(d_proj, student_out, preferred_element_type=jnp.float32).astype(jnp.bfloat16)
        d_attn = d_attn.reshape(SEQ, HEADS, HS).astype(jnp.float32)
        d_prob = jnp.einsum('qhd,khd->hqk', d_attn, values.astype(jnp.float32))
        d_score = (weights * (d_prob - lax.optimization_barrier(jnp.sum(weights * d_prob, axis=-1, keepdims=True))) / math.sqrt(HS)).astype(jnp.bfloat16)
        d_score = d_score.astype(jnp.float32)
        d_query = jnp.einsum('hqk,khd->qhd', d_score, keys_all.astype(jnp.float32)).astype(jnp.bfloat16)
        d_key = jnp.einsum('hqk,qhd->khd', d_score, queries.astype(jnp.float32)).astype(jnp.bfloat16)
        d_value = jnp.einsum('hqk,qhd->khd', rounded.astype(jnp.float32), d_attn).astype(jnp.bfloat16)
        d_pack = jnp.stack([d_query, d_key, d_value], axis=1).reshape(SEQ, 3 * INNER)
        grad_qkv = lax.dot_general(shaped, d_pack, (((0,), (0,)), ((), ())), preferred_element_type=jnp.float32)
        return ((carry[0] + grad_qkv, carry[1] + grad_out, carry[2] + sample_loss), None)
    start_carry = (jnp.zeros((D, 3 * INNER), jnp.float32), jnp.zeros((D, INNER), jnp.float32), jnp.zeros((), jnp.float32))
    sums, unused = lax.scan(sample_step, start_carry, (clean_latent, noise_draw, timestep, bucket))
    grad_qkv = sums[0].reshape(D, 3, INNER)
    grad_out = sums[1]
    squares = jnp.sum(grad_qkv * grad_qkv) + jnp.sum(grad_out * grad_out)
    rms_value = jnp.sqrt(squares / (4 * D * INNER))
    factor = 1.0 / jnp.maximum(rms_value, 1.0)

    def adam(moment, second, grad):
        normed_grad = grad * factor
        new_moment = BETA_ONE * moment + (1.0 - BETA_ONE) * normed_grad
        new_second = BETA_TWO * second + (1.0 - BETA_TWO) * normed_grad * normed_grad
        return (new_moment, new_second, new_moment / (jnp.sqrt(new_second) + ADAM_EPS))
    mq, vq, uq = adam(moment_qkv, second_qkv, grad_qkv)
    mo, vo, uo = adam(moment_out, second_out, grad_out)
    loss = sums[2] / (SAMPLES * LATENT)
    return (mq, vq, uq, mo, vo, uo, loss)
```

```python
import math

import jax
import jax.numpy as jnp
import numpy as np
from jax import lax
from jax.experimental import pallas as pl
from jax.experimental.pallas import tpu as pltpu
from jax.sharding import Mesh
from jax.sharding import PartitionSpec as P

HS = 64
PATCH_CH = 16
TGRID = 16
LN_EPS = 0.01
BETA_ONE = 0.9
BETA_TWO = 0.99
ADAM_EPS = 1e-08

LANES = 128
PAD = 16
STEP = 16
UNROLL = 4
F32 = jnp.float32
BF16 = jnp.bfloat16
VMEM_LIMIT = 58 * 1024 * 1024


def position_tables(seq, width):
    half = width // 2
    freqs = np.exp(-math.log(10000.0) * np.arange(half, dtype=np.float64) / half)
    coarse = 8.0 * np.arange(seq // 8)[:, None] * freqs[None, :]
    fine = np.arange(8.0)[:, None] * freqs[None, :]
    return (
        np.stack([np.sin(coarse), np.cos(coarse)]).astype(np.float32),
        np.stack([np.sin(fine), np.cos(fine)]).astype(np.float32),
    )


def dot(a, b):
    return jnp.dot(a, b, preferred_element_type=F32)


def dot_t(a, b):
    return lax.dot_general(a, b, (((1,), (1,)), ((), ())), preferred_element_type=F32)


def dot_c(a, b):
    return lax.dot_general(a, b, (((0,), (0,)), ((), ())), preferred_element_type=F32)


def split3(x):
    one = x.astype(BF16).astype(F32)
    rest = x - one
    two = rest.astype(BF16).astype(F32)
    return (one, two, (rest - two).astype(BF16).astype(F32))


def left_parts(x):
    one, two, three = split3(x)
    return jnp.concatenate([one, one, one, two, two, three], axis=1).astype(BF16)


def right_parts(w):
    one, two, three = split3(w)
    return jnp.concatenate([one, two, three, one, two, one], axis=0).astype(BF16)


def unpack_tokens(packed):
    return jnp.concatenate(
        [packed[:, PATCH_CH * b : PATCH_CH * (b + 1)] for b in range(8)], axis=0
    )


def level(tau):
    lamb = 6.0 - 12.0 * (jnp.zeros((1, LANES), F32) + tau.astype(F32)) / TGRID
    alpha = jnp.sqrt(1.0 / (1.0 + jnp.exp(-lamb)))
    sigma = jnp.sqrt(1.0 / (1.0 + jnp.exp(lamb)))
    return (alpha, sigma)


def norm_rows(low, high, width):
    mean = (jnp.sum(low, 1, keepdims=True) + jnp.sum(high, 1, keepdims=True)) / width
    low = low - mean
    high = high - mean
    square = jnp.sum(low * low, 1, keepdims=True) + jnp.sum(high * high, 1, keepdims=True)
    inverse = lax.rsqrt(square / width + LN_EPS)
    return (low * inverse, high * inverse, inverse)


def position_rows(coarse, fine, start, seq):
    per = seq // 8
    b = start // per
    a = pl.multiple_of(start % per, STEP)
    sa = coarse[0, pl.ds(a, STEP), :]
    ca = coarse[1, pl.ds(a, STEP), :]
    sb = fine[0, pl.ds(b, 1), :]
    cb = fine[1, pl.ds(b, 1), :]
    return (sa * cb + ca * sb, ca * cb - sa * sb)


def mod_row(table, which, index):
    return table[which, pl.ds(index, 1), :]


def attention_pair(q, k, v):
    lane = lax.broadcasted_iota(jnp.int32, (1, LANES), 1)
    lower = (lane < HS).astype(F32)
    parts = []
    for mask in (lower, 1.0 - lower):
        scores = dot_t(q * mask.astype(BF16), k) * (1.0 / math.sqrt(HS))
        top = jnp.max(scores, axis=-1, keepdims=True)
        expos = jnp.exp(scores - top)
        weights = expos * (1.0 / jnp.sum(expos, axis=-1, keepdims=True))
        parts.append(weights)
    return (parts, lower)


def quantize(x, ref, lead):
    top = jnp.maximum(jnp.max(jnp.abs(x), axis=0, keepdims=True), 1e-30)
    code = jnp.ceil(jnp.log(top) * (256.0 / math.log(2.0)))
    scale = jnp.exp(code * (math.log(2.0) / 256.0))
    rows = x.shape[0]
    ref[lead, 0:rows, :] = jnp.round(x * (32700.0 / scale)).astype(jnp.int32).astype(jnp.int16)
    ref[lead, rows : rows + PAD, :] = (
        jnp.broadcast_to(code, (PAD, x.shape[1])).astype(jnp.int32).astype(jnp.int16)
    )


def restore(ref, lead, rows):
    code = ref[lead, rows : rows + PAD, :].astype(jnp.int32).astype(F32)[0:1]
    scale = jnp.exp(code * (math.log(2.0) / 256.0)) * (1.0 / 32700.0)
    return ref[lead, 0:rows, :].astype(jnp.int32).astype(F32) * scale


VM = pl.BlockSpec(memory_space=pltpu.VMEM)
SM = pl.BlockSpec(memory_space=pltpu.SMEM)
ANY = pl.BlockSpec(memory_space=pl.ANY)


def call(body, outs, ins, scratch, flops, name, after=()):
    out_shape = [jax.ShapeDtypeStruct(s, d) for s, d in outs]
    moved = sum(math.prod(s) * jnp.dtype(d).itemsize for s, d in outs)
    moved += sum(a.size * a.dtype.itemsize for _, a in ins)
    n, k = len(ins), len(after)

    def kernel(*refs):
        body(*refs[:n], *refs[n + k :])

    return pl.pallas_call(
        kernel,
        out_shape=out_shape,
        in_specs=[s for s, _ in ins] + [ANY] * k,
        out_specs=[VM] * len(outs),
        scratch_shapes=scratch,
        compiler_params=pltpu.CompilerParams(vmem_limit_bytes=VMEM_LIMIT),
        cost_estimate=pl.CostEstimate(
            flops=int(flops), bytes_accessed=int(moved), transcendentals=0
        ),
        name=name,
    )(*[a for _, a in ins], *after)


def all_sum(x, axis, n):
    if n & (n - 1):
        return x + sum(shift(x, axis, n, s) for s in range(1, n))
    bit = 1
    while bit < n:
        x = x + lax.ppermute(x, axis, [(k, k ^ bit) for k in range(n)])
        bit *= 2
    return x


def shift(x, axis, n, s):
    return lax.ppermute(x, axis, [(k, (k + s) % n) for k in range(n)])


def make_step(groups, peers, halves, dp):
    def step(
        clean_latent,
        noise_draw,
        timestep,
        bucket,
        bucket_weights,
        teacher_embed,
        teacher_final,
        teacher_mod,
        teacher_qkv,
        teacher_out,
        student_embed,
        student_final,
        student_mod,
        student_qkv,
        student_out,
        moment_qkv,
        second_qkv,
        moment_out,
        second_out,
    ):
        G, R, M = groups, peers, halves
        width, inner = teacher_out.shape
        samples, latent = clean_latent.shape
        assert samples == 1
        seq = latent // PATCH_CH
        packed_rows = latent // LANES
        own = student_out.shape[0]
        half = seq // M
        W = width // 2
        cols = 3 * LANES
        z = lax.axis_index("dz")
        r = lax.axis_index("dr")
        m = lax.axis_index("mp")
        ids = jnp.concatenate(
            [timestep, bucket, jnp.stack([z, r, m]).astype(jnp.int32)]
        )
        coarse_np, fine_np = position_tables(seq, width)
        coarse = jnp.asarray(coarse_np)
        fine = jnp.asarray(fine_np)
        clean = clean_latent.reshape(packed_rows, LANES)
        noise = noise_draw.reshape(packed_rows, LANES)
        tmod = jnp.transpose(teacher_mod, (1, 0, 2))
        smod = jnp.transpose(student_mod, (1, 0, 2))
        tqkv = jnp.transpose(teacher_qkv, (1, 0, 2))
        sqkv = jnp.transpose(student_qkv, (1, 0, 2))
        chunk_rows = 3 * own
        extra = 3 * packed_rows + PAD

        def prologue(ids_ref, clean_ref, noise_ref, qkv_ref, *outs):
            first = 2 * ids_ref[0]
            alpha, sigma = level(first)
            lat = alpha * clean_ref[...] + sigma * noise_ref[...]
            parts = split3(lat)
            for s in range(G):
                to = lax.rem(ids_ref[2] + s, G)
                lanes = pl.ds(pl.multiple_of(to * LANES, LANES), LANES)
                for t in range(3):
                    outs[s][t * own : (t + 1) * own, :] = qkv_ref[t, :, lanes]
                for j in range(3):
                    base = chunk_rows + j * packed_rows
                    outs[s][base : base + packed_rows, :] = parts[j].astype(BF16)
                outs[s][chunk_rows + 3 * packed_rows :, :] = jnp.full(
                    (PAD, LANES), 1.0, F32
                ).astype(BF16) * (ids_ref[0].astype(F32)).astype(BF16)

        pieces = call(
            prologue,
            [((chunk_rows + extra, LANES), BF16)] * G,
            [(SM, ids), (VM, clean), (VM, noise), (VM, sqkv)],
            [],
            1e6,
            "prologue",
        )
        got = [pieces[0]] + [shift(pieces[s], "dz", G, s) for s in range(1, G)]
        out_got = [student_out] + [shift(student_out, "dz", G, s) for s in range(1, G)]
        bundle = jnp.stack([g[:chunk_rows] for g in got])
        bundles = [bundle] + [shift(bundle, "dr", R, s) for s in range(1, R)]
        out_bundle = jnp.stack(out_got)
        out_bundles = [out_bundle] + [shift(out_bundle, "dr", R, s) for s in range(1, R)]

        def place(ids_ref, s, y):
            rr = lax.rem(ids_ref[3] + (R - s), R)
            zz = lax.rem(ids_ref[2] + (G - y), G)
            return pl.ds(pl.multiple_of((zz * R + rr) * own, own), own)

        def spread(ids_ref, parts, target):
            for s in range(M):
                at = pl.multiple_of(lax.rem(ids_ref[4] + (M - s), M) * half, half)
                target[pl.ds(at, half), :] = parts[s][...]

        def teacher_front(is_first, lat_arrays):
            def body(*refs):
                ids_ref = refs[0]
                lat_refs = refs[1 : 1 + len(lat_arrays)]
                embed, mod, w_hbm, o_hbm, coarse_r, fine_r = refs[
                    1 + len(lat_arrays) : 7 + len(lat_arrays)
                ]
                rest = refs[7 + len(lat_arrays) :]
                n_out = M + (1 if is_first else 0)
                outs = rest[:n_out]
                w_v, o_v, hid, shaped, qkv_s, att, sems, lat_v = rest[n_out:]
                loads = [
                    pltpu.make_async_copy(w_hbm.at[t], w_v.at[t], sems.at[t]) for t in range(3)
                ]
                loads.append(pltpu.make_async_copy(o_hbm, o_v, sems.at[3]))
                for c in loads:
                    c.start()
                first = 2 * ids_ref[0]
                if is_first:
                    alpha, sigma = level(first)
                    lat = unpack_tokens(alpha * lat_refs[0][...] + sigma * lat_refs[1][...])
                    outs[M][...] = lat
                    index = first - 1
                else:
                    spread(ids_ref, lat_refs, lat_v)
                    lat = lat_v[...]
                    index = first - 2
                hid[...] = dot(left_parts(lat), right_parts(embed[...]))
                shift_row = mod_row(mod, 0, index)
                scale_row = 1.0 + mod_row(mod, 1, index)
                gate_row = mod_row(mod, 2, index)

                def rows(i, _):
                    start = pl.multiple_of(i * STEP, STEP)
                    sin, cos = position_rows(coarse_r, fine_r, start, seq)
                    low = hid[pl.ds(start, STEP), 0:W] + sin
                    high = hid[pl.ds(start, STEP), W:] + cos
                    hid[pl.ds(start, STEP), 0:W] = low
                    hid[pl.ds(start, STEP), W:] = high
                    low, high, _ = norm_rows(low, high, width)
                    shaped[pl.ds(start, STEP), 0:W] = (
                        low * scale_row[:, 0:W] + shift_row[:, 0:W]
                    ).astype(BF16)
                    shaped[pl.ds(start, STEP), W:] = (
                        high * scale_row[:, W:] + shift_row[:, W:]
                    ).astype(BF16)
                    return 0

                lax.fori_loop(0, seq // STEP, rows, 0, unroll=UNROLL)
                for t in range(3):
                    loads[t].wait()
                    qkv_s[t] = dot(shaped[...], w_v[t]).astype(BF16)
                for p in range(inner // LANES):
                    lanes = slice(p * LANES, (p + 1) * LANES)
                    v = qkv_s[2, :, lanes]
                    weights, lower = attention_pair(qkv_s[0, :, lanes], qkv_s[1, :, lanes], v)
                    low = dot(weights[0].astype(BF16), v)
                    high = dot(weights[1].astype(BF16), v)
                    att[:, lanes] = (low * lower + high * (1.0 - lower)).astype(BF16)
                loads[3].wait()
                for s in range(1, M):
                    at = pl.multiple_of(lax.rem(ids_ref[4] + s, M) * half, half)
                    outs[s][...] = dot_t(att[pl.ds(at, half), :], o_v[...])
                mine = pl.multiple_of(ids_ref[4] * half, half)
                outs[0][...] = hid[pl.ds(mine, half), :] + gate_row * dot_t(
                    att[pl.ds(mine, half), :], o_v[...]
                )

            outs = [((half, width), F32)] * M
            if is_first:
                outs = outs + [((seq, PATCH_CH), F32)]
            return call(
                body,
                outs,
                [(SM, ids)]
                + [(VM, a) for a in lat_arrays]
                + [
                    (VM, teacher_embed),
                    (VM, tmod),
                    (ANY, tqkv),
                    (ANY, teacher_out),
                    (VM, coarse),
                    (VM, fine),
                ],
                [
                    pltpu.VMEM((3, width, inner), BF16),
                    pltpu.VMEM((width, inner), BF16),
                    pltpu.VMEM((seq, width), F32),
                    pltpu.VMEM((seq, width), BF16),
                    pltpu.VMEM((3, seq, inner), BF16),
                    pltpu.VMEM((seq, inner), BF16),
                    pltpu.SemaphoreType.DMA((4,)),
                    pltpu.VMEM((seq, PATCH_CH), F32),
                ],
                2 * seq * width * inner * 4,
                "teacher_front_first" if is_first else "teacher_front_second",
            )

        def exchange(outs):
            return [outs[0]] + [shift(outs[s], "mp", M, s) for s in range(1, M)]

        def tail_rows(mixed_refs, gate_row, parts_ref, norm_ref, inv_ref):
            def rows(i, _):
                start = pl.multiple_of(i * STEP, STEP)
                more_low = mixed_refs[1][pl.ds(start, STEP), 0:W]
                more_high = mixed_refs[1][pl.ds(start, STEP), W:]
                for ref in mixed_refs[2:]:
                    more_low = more_low + ref[pl.ds(start, STEP), 0:W]
                    more_high = more_high + ref[pl.ds(start, STEP), W:]
                low = mixed_refs[0][pl.ds(start, STEP), 0:W] + gate_row[:, 0:W] * more_low
                high = mixed_refs[0][pl.ds(start, STEP), W:] + gate_row[:, W:] * more_high
                low, high, inverse = norm_rows(low, high, width)
                if norm_ref is not None:
                    norm_ref[pl.ds(start, STEP), 0:W] = low
                    norm_ref[pl.ds(start, STEP), W:] = high
                    inv_ref[pl.ds(start, STEP), :] = jnp.broadcast_to(inverse, (STEP, LANES))
                for j, (a, b) in enumerate(zip(split3(low), split3(high))):
                    parts_ref[j, pl.ds(start, STEP), 0:W] = a.astype(BF16)
                    parts_ref[j, pl.ds(start, STEP), W:] = b.astype(BF16)
                return 0

            lax.fori_loop(0, half // STEP, rows, 0, unroll=UNROLL)

        def project(parts_ref, final_ref):
            f = jnp.concatenate(split3(final_ref[...]), axis=0).astype(BF16)
            C = PATCH_CH
            a = dot_t(parts_ref[0], f)
            b = dot_t(parts_ref[1], f)
            c = dot_t(parts_ref[2], f)
            tiny = a[:, 2 * C : 3 * C] + b[:, C : 2 * C] + c[:, 0:C]
            return (tiny + (a[:, C : 2 * C] + b[:, 0:C])) + a[:, 0:C]

        def narrow(pair):
            return tuple(x[:, 0:PATCH_CH] for x in pair)

        def teacher_tail(is_first, mixed, lat0, lat1=None, after=()):
            def body(ids_ref, *refs):
                mixed_refs = refs[:M]
                mod, final, lat_ref = refs[M : M + 3]
                out, parts = refs[-2:]
                first = 2 * ids_ref[0]
                index = first - 1 if is_first else first - 2
                tail_rows(mixed_refs, mod_row(mod, 2, index), parts, None, None)
                eps = project(parts, final)
                mine = pl.multiple_of(ids_ref[4] * half, half)
                latent0 = lat_ref[pl.ds(mine, half), :]
                af, sf = narrow(level(first))
                am, sm = narrow(level(first - 1))
                if is_first:
                    out[...] = am * (latent0 - sf * eps) / af + sm * eps
                else:
                    al, sl = narrow(level(first - 2))
                    latent2 = al * (refs[M + 3][...] - sm * eps) / am + sl * eps
                    out[...] = (latent0 - af / al * latent2) / (sf - af * sl / al)

            return call(
                body,
                [((half, PATCH_CH), F32)],
                [(SM, ids)]
                + [(VM, a) for a in mixed]
                + [(VM, tmod), (VM, teacher_final), (VM, lat0)]
                + ([] if is_first else [(VM, lat1)]),
                [pltpu.VMEM((3, half, width), BF16)],
                1e9,
                "teacher_tail_first" if is_first else "teacher_tail_second",
                after,
            )[0]

        def student_front(after):
            def body(ids_ref, embed, mod, coarse_r, fine_r, *refs):
                bun = refs[:R]
                lats = refs[R : R + G]
                atts = refs[R + G : R + 2 * G]
                qkv_o, shaped_o = refs[R + 2 * G : R + 2 * G + 2]
                w_v, hid = refs[R + 2 * G + 2 :]
                for s in range(R):
                    for y in range(G):
                        at = place(ids_ref, s, y)
                        for t in range(3):
                            w_v[at, t * LANES : (t + 1) * LANES] = bun[s][
                                y, t * own : (t + 1) * own, :
                            ]
                right = right_parts(embed[...])
                for y in range(G):
                    one, two, three = (
                        unpack_tokens(
                            lats[y][
                                chunk_rows + j * packed_rows : chunk_rows + (j + 1) * packed_rows, :
                            ].astype(F32)
                        )
                        for j in range(3)
                    )
                    left = jnp.concatenate([one, one, one, two, two, three], axis=1)
                    hid[...] = dot(left.astype(BF16), right)
                    step_of = lats[y][chunk_rows + 3 * packed_rows :, :].astype(F32)
                    count = mod.shape[1]
                    shift_row = jnp.zeros((1, width), F32)
                    scale_row = jnp.zeros((1, width), F32)
                    for k in range(count):
                        hit = (step_of[0:1, 0:1] == float(k + 1))
                        shift_row = jnp.where(hit, mod[0, k : k + 1, :], shift_row)
                        scale_row = jnp.where(hit, mod[1, k : k + 1, :], scale_row)
                    scale_row = 1.0 + scale_row

                    def rows(i, _, y=y, shift_row=shift_row, scale_row=scale_row):
                        start = pl.multiple_of(i * STEP, STEP)
                        sin, cos = position_rows(coarse_r, fine_r, start, seq)
                        low = hid[pl.ds(start, STEP), 0:W] + sin
                        high = hid[pl.ds(start, STEP), W:] + cos
                        low, high, _ = norm_rows(low, high, width)
                        shaped_o[y, pl.ds(start, STEP), 0:W] = (
                            low * scale_row[:, 0:W] + shift_row[:, 0:W]
                        ).astype(BF16)
                        shaped_o[y, pl.ds(start, STEP), W:] = (
                            high * scale_row[:, W:] + shift_row[:, W:]
                        ).astype(BF16)
                        return 0

                    lax.fori_loop(0, seq // STEP, rows, 0, unroll=UNROLL)
                    qkv_o[y] = dot(shaped_o[y], w_v[...]).astype(BF16)
                    v = qkv_o[y, :, 2 * LANES :]
                    weights, lower = attention_pair(
                        qkv_o[y, :, 0:LANES], qkv_o[y, :, LANES : 2 * LANES], v
                    )
                    low = dot(weights[0].astype(BF16), v)
                    high = dot(weights[1].astype(BF16), v)
                    atts[y][...] = (low * lower + high * (1.0 - lower)).astype(BF16)

            return call(
                body,
                [((seq, LANES), BF16)] * G
                + [
                    ((G, seq, cols), BF16),
                    ((G, seq, width), BF16),
                ],
                [(SM, ids), (VM, student_embed), (VM, smod), (VM, coarse), (VM, fine)]
                + [(VM, b) for b in bundles]
                + [(VM, a) for a in got],
                [pltpu.VMEM((width, cols), BF16), pltpu.VMEM((seq, width), F32)],
                2 * G * seq * width * cols,
                "student_front",
                after,
            )

        def student_out_proj(att_pieces, lat0):
            def body(ids_ref, embed, mod, coarse_r, fine_r, lat_ref, *refs):
                pieces_r = refs[:G]
                bun = refs[G : G + R]
                refs = refs[G + R :]
                outs = refs[:M]
                att_o, out_w, hid = refs[M:]
                for s in range(R):
                    for y in range(G):
                        out_w[place(ids_ref, s, y), :] = bun[s][y]
                for s in range(G):
                    at = pl.multiple_of(lax.rem(ids_ref[2] + s, G) * LANES, LANES)
                    att_o[:, pl.ds(at, LANES)] = pieces_r[s][...]
                for s in range(1, M):
                    at = pl.multiple_of(lax.rem(ids_ref[4] + s, M) * half, half)
                    outs[s][...] = dot_t(att_o[pl.ds(at, half), :], out_w[...])
                mine = pl.multiple_of(ids_ref[4] * half, half)
                hid[...] = dot_t(att_o[pl.ds(mine, half), :], out_w[...])
                outs[0][...] = dot(
                    left_parts(lat_ref[pl.ds(mine, half), :]), right_parts(embed[...])
                )
                gate_row = mod_row(mod, 2, ids_ref[0] - 1)

                def rows(i, _):
                    start = pl.multiple_of(i * STEP, STEP)
                    sin, cos = position_rows(coarse_r, fine_r, mine + start, seq)
                    at = pl.ds(start, STEP)
                    outs[0][at, 0:W] = (
                        outs[0][at, 0:W] + sin + gate_row[:, 0:W] * hid[at, 0:W]
                    )
                    outs[0][at, W:] = outs[0][at, W:] + cos + gate_row[:, W:] * hid[at, W:]
                    return 0

                lax.fori_loop(0, half // STEP, rows, 0, unroll=UNROLL)

            return call(
                body,
                [((half, width), F32)] * M + [((seq, inner), BF16), ((width, inner), BF16)],
                [
                    (SM, ids),
                    (VM, student_embed),
                    (VM, smod),
                    (VM, coarse),
                    (VM, fine),
                    (VM, lat0),
                ]
                + [(VM, a) for a in att_pieces]
                + [(VM, a) for a in out_bundles],
                [pltpu.VMEM((half, width), F32)],
                2 * seq * width * inner,
                "student_out_proj",
            )

        def last_tail(student_mixed, goal):
            def body(ids_ref, bw_ref, *refs):
                s_refs = refs[:M]
                sm_table, sf_w, goal_r, dproj, loss = refs[M : M + 5]
                parts, normed, inv, grad = refs[M + 5 :]
                target = goal_r[...]
                gate_row = mod_row(sm_table, 2, ids_ref[0] - 1)
                tail_rows(s_refs, gate_row, parts, normed, inv)
                error = project(parts, sf_w) - target
                weight = bw_ref[ids_ref[1]]
                loss[...] = jnp.broadcast_to(
                    weight * jnp.sum(jnp.sum(error * error, 1, keepdims=True), 0, keepdims=True),
                    (8, LANES),
                )
                grad[...] = dot(left_parts(2.0 * weight * error), right_parts(sf_w[...]))

                def rows(i, _):
                    start = pl.multiple_of(i * STEP, STEP)
                    at = pl.ds(start, STEP)
                    ul, uh = grad[at, 0:W], grad[at, W:]
                    nl, nh = normed[at, 0:W], normed[at, W:]
                    one = (jnp.sum(ul, 1, keepdims=True) + jnp.sum(uh, 1, keepdims=True)) / width
                    two = (
                        jnp.sum(ul * nl, 1, keepdims=True) + jnp.sum(uh * nh, 1, keepdims=True)
                    ) / width
                    inverse = inv[at, 0:1]
                    dproj[at, 0:W] = (
                        gate_row[:, 0:W] * ((ul - one - nl * two) * inverse)
                    ).astype(BF16)
                    dproj[at, W:] = (
                        gate_row[:, W:] * ((uh - one - nh * two) * inverse)
                    ).astype(BF16)
                    return 0

                lax.fori_loop(0, half // STEP, rows, 0, unroll=UNROLL)

            return call(
                body,
                [((half, width), BF16), ((8, LANES), F32)],
                [(SM, ids), (SM, bucket_weights)]
                + [(VM, a) for a in student_mixed]
                + [(VM, smod), (VM, student_final), (VM, goal)],
                [
                    pltpu.VMEM((3, half, width), BF16),
                    pltpu.VMEM((half, width), F32),
                    pltpu.VMEM((half, LANES), F32),
                    pltpu.VMEM((half, width), F32),
                ],
                3e9,
                "last_tail",
            )

        def back_out(d_proj, out_full):
            def body(ids_ref, out_w, *refs):
                outs = refs[M : M + G]
                (full,) = refs[M + G :]
                for s in range(M):
                    at = pl.multiple_of(lax.rem(ids_ref[4] + (M - s), M) * half, half)
                    full[pl.ds(at, half), :] = dot(refs[s][...], out_w[...]).astype(BF16)
                for s in range(G):
                    at = pl.multiple_of(lax.rem(ids_ref[2] + s, G) * LANES, LANES)
                    outs[s][...] = full[:, pl.ds(at, LANES)]

            return call(
                body,
                [((seq, LANES), BF16)] * G,
                [(SM, ids), (VM, out_full)] + [(VM, a) for a in d_proj],
                [pltpu.VMEM((seq, inner), BF16)],
                2 * seq * width * inner,
                "back_out",
            )

        def emit(ids_ref, full, outs):
            for s in range(R):
                rr = lax.rem(ids_ref[3] + s, R)
                for y in range(G):
                    at = pl.multiple_of((y * R + rr) * own, own)
                    block = full[pl.ds(at, own), :]
                    if s == 0:
                        outs[0][y] = block
                    else:
                        quantize(block, outs[s], y)

        def payloads(n):
            return [((G, own, n), F32)] + [((G, own + PAD, n), jnp.int16)] * (R - 1)

        def grad_out_kernel(d_proj, attended, after):
            def body(ids_ref, att_ref, *refs):
                outs = refs[M : M + R]
                full, both = refs[M + R :]
                spread(ids_ref, refs[:M], both)
                full[...] = dot_c(both[...], att_ref[...])
                emit(ids_ref, full, outs)

            return call(
                body,
                payloads(inner),
                [(SM, ids), (VM, attended)] + [(VM, a) for a in d_proj],
                [pltpu.VMEM((width, inner), F32), pltpu.VMEM((seq, width), BF16)],
                2 * seq * width * inner,
                "grad_out",
                after,
            )

        def back_attention(d_atts, packed, shaped):
            def body(ids_ref, qkv_r, shaped_r, *refs):
                da = refs[:G]
                outs = refs[G : G + R]
                full, pack = refs[G + R :]
                for y in range(G):
                    q = qkv_r[y, :, 0:LANES]
                    k = qkv_r[y, :, LANES : 2 * LANES]
                    v = qkv_r[y, :, 2 * LANES :]
                    weights, lower = attention_pair(q, k, v)
                    d_att = da[y][...]
                    sums = [None, None, None]
                    for h in range(2):
                        mask = lower if h == 0 else 1.0 - lower
                        w = weights[h]
                        d_prob = dot_t(d_att * mask.astype(BF16), v)
                        inside = jnp.sum(w * d_prob, axis=-1, keepdims=True)
                        d_score = (w * (d_prob - inside) * (1.0 / math.sqrt(HS))).astype(BF16)
                        got3 = (
                            dot(d_score, k),
                            dot_c(d_score, q),
                            dot_c(w.astype(BF16), d_att),
                        )
                        for j in range(3):
                            part = got3[j] * mask
                            sums[j] = part if h == 0 else sums[j] + part
                    for j in range(3):
                        pack[:, j * LANES : (j + 1) * LANES] = sums[j].astype(BF16)
                    part = dot_c(shaped_r[y], pack[...])
                    if y == 0:
                        full[...] = part
                    else:
                        full[...] += part
                emit(ids_ref, full, outs)

            return call(
                body,
                payloads(cols),
                [(SM, ids), (VM, packed), (VM, shaped)] + [(VM, a) for a in d_atts],
                [pltpu.VMEM((width, cols), F32), pltpu.VMEM((seq, cols), BF16)],
                2 * G * seq * width * cols,
                "back_attention",
            )

        def fold(own_r, others, full):
            acc = None
            for y in range(G):
                x = own_r[y]
                for ref in others:
                    x = x + restore(ref, y, own)
                full[y] = x
                part = jnp.sum(x * x, axis=0, keepdims=True)
                acc = part if acc is None else acc + part
            return jnp.sum(acc, 1, keepdims=True)

        def hand_on(ids_ref, full, outs):
            for s in range(G):
                block = full[lax.rem(ids_ref[2] + s, G)]
                if s == 0:
                    outs[0][...] = block
                else:
                    quantize(block, outs[s], 0)

        def passed(n):
            return [((own, n), F32)] + [((1, own + PAD, n), jnp.int16)] * (G - 1)

        def out_sum(mine, received):
            def body(ids_ref, *refs):
                outs = refs[R : R + G]
                full = refs[-1]
                fold(refs[0], refs[1:R], full)
                hand_on(ids_ref, full, outs)

            return call(
                body,
                passed(inner),
                [(SM, ids), (VM, mine)] + [(VM, a) for a in received],
                [pltpu.VMEM((G, own, inner), F32)],
                1e8,
                "out_sum",
            )

        def last_sum(mine, received, out_parts, loss_part):
            def body(ids_ref, loss_r, *refs):
                o_parts = refs[:G]
                refs = refs[G:]
                outs = refs[R : R + G]
                grad_o, total, full = refs[R + G :]
                squares = fold(refs[0], refs[1:R], full)
                hand_on(ids_ref, full, outs)
                x = o_parts[0][...]
                for ref in o_parts[1:]:
                    x = x + restore(ref, 0, own)
                grad_o[...] = x
                more = jnp.sum(jnp.sum(x * x, axis=0, keepdims=True), 1, keepdims=True)
                total[0:8, :] = jnp.broadcast_to(squares + more, (8, LANES))
                total[8:16, :] = loss_r[...]

            return call(
                body,
                passed(cols) + [((own, inner), F32), ((16, LANES), F32)],
                [(SM, ids), (VM, loss_part)]
                + [(VM, a) for a in out_parts]
                + [(VM, mine)]
                + [(VM, a) for a in received],
                [pltpu.VMEM((G, own, cols), F32)],
                1e8,
                "last_sum",
            )

        def adam_kernel(total, qkv_parts, grad_out, state):
            def body(ids_ref, total_r, *refs):
                parts = refs[:G]
                go, mq, vq, mo, vo = refs[G : G + 5]
                nmq, nvq, uq, nmo, nvo, uo = refs[G + 5 : G + 11]
                (grad,) = refs[G + 11 :]
                rms = jnp.sqrt(total_r[0:1, 0:1] / (4 * width * inner * M))
                factor = 1.0 / jnp.maximum(rms, 1.0)
                for s in range(G):
                    at = pl.multiple_of(lax.rem(ids_ref[2] + (G - s), G) * LANES, LANES)
                    block = parts[s][...] if s == 0 else restore(parts[s], 0, own)
                    for t in range(3):
                        grad[t, :, pl.ds(at, LANES)] = block[:, t * LANES : (t + 1) * LANES]

                def adam(g, moment, second):
                    g = g * factor
                    moment = BETA_ONE * moment + (1.0 - BETA_ONE) * g
                    second = BETA_TWO * second + (1.0 - BETA_TWO) * g * g
                    return (moment, second, moment / (jnp.sqrt(second) + ADAM_EPS))

                for t in range(3):
                    nmq[t], nvq[t], uq[t] = adam(grad[t], mq[t], vq[t])
                nmo[...], nvo[...], uo[...] = adam(go[...], mo[...], vo[...])

            return call(
                body,
                [((3, own, inner), F32)] * 3 + [((own, inner), F32)] * 3,
                [(SM, ids), (VM, total)]
                + [(VM, a) for a in qkv_parts]
                + [(VM, grad_out)]
                + [(VM, a) for a in state],
                [pltpu.VMEM((3, own, inner), F32)],
                1e8,
                "adam",
            )

        def whole(part):
            return [part] + [shift(part, "mp", M, s) for s in range(1, M)]

        *mixed_a, lat0 = teacher_front(True, [clean, noise])
        mixed_a = exchange(mixed_a)
        next_mine = teacher_tail(True, mixed_a, lat0)
        mixed_b = teacher_front(False, whole(next_mine))
        *att_out, packed, shaped = student_front((mixed_b[0],))
        mixed_b = exchange(mixed_b)
        att_pieces = [att_out[0]] + [shift(att_out[s], "dz", G, -s) for s in range(1, G)]
        goal = teacher_tail(False, mixed_b, lat0, next_mine, (att_out[0],))
        *mixed_s, attended, out_full = student_out_proj(att_pieces, lat0)
        mixed_s = exchange(mixed_s)
        d_proj_mine, loss_part = last_tail(mixed_s, goal)
        d_proj = whole(d_proj_mine)
        d_out = back_out(d_proj, out_full)
        d_atts = [d_out[0]] + [shift(d_out[s], "dz", G, s) for s in range(1, G)]
        go = grad_out_kernel(d_proj, attended, (d_out[0],))
        go_recv = [shift(go[s], "dr", R, s) for s in range(1, R)]
        gq = back_attention(d_atts, packed, shaped)
        gq_recv = [shift(gq[s], "dr", R, s) for s in range(1, R)]
        go_z = out_sum(go[0], go_recv)
        out_parts = [go_z[0]] + [shift(go_z[s], "dz", G, s) for s in range(1, G)]
        *gq_z, grad_out, both = last_sum(gq[0], gq_recv, out_parts, loss_part)
        qkv_parts = [gq_z[0]] + [shift(gq_z[s], "dz", G, s) for s in range(1, G)]
        for axis, n in (("mp", M), ("dr", R), ("dz", G)):
            both = all_sum(both, axis, n)
        view = lambda a: jnp.transpose(a, (1, 0, 2))
        nmq, nvq, uq, nmo, nvo, uo = adam_kernel(
            both,
            qkv_parts,
            grad_out,
            [view(moment_qkv), view(second_qkv), moment_out, second_out],
        )
        loss = both[8, 0] / (samples * dp * latent)
        return (view(nmq), view(nvq), view(uq), nmo, nvo, uo, loss)

    return step


def solution(mesh):
    dp, halves = mesh.shape["dp"], mesh.shape["mp"]

    def run(*args):
        groups = args[9].shape[1] // halves // LANES
        peers = dp // groups
        fine = Mesh(mesh.devices.reshape(groups, peers, halves), ("dz", "dr", "mp"))
        dd = ("dz", "dr")
        specs = (
            P(dd, None),
            P(dd, None),
            P(dd),
            P(dd),
            P(),
            P(),
            P(),
            P(),
            P(None, None, "mp"),
            P(None, "mp"),
            P(),
            P(),
            P(),
            P(dd, None, "mp"),
            P(dd, "mp"),
            P(dd, None, "mp"),
            P(dd, None, "mp"),
            P(dd, "mp"),
            P(dd, "mp"),
        )
        return jax.shard_map(
            make_step(groups, peers, halves, dp),
            mesh=fine,
            in_specs=specs,
            out_specs=(
                P(dd, None, "mp"),
                P(dd, None, "mp"),
                P(dd, None, "mp"),
                P(dd, "mp"),
                P(dd, "mp"),
                P(dd, "mp"),
                P(),
            ),
            check_vma=False,
        )(*args)

    return run
```

```python
import math

import jax
import jax.numpy as jnp
import numpy as np
from jax import lax
from jax.experimental import pallas as pl
from jax.experimental.pallas import tpu as pltpu
from jax.sharding import Mesh
from jax.sharding import PartitionSpec as P


HS = 64
PATCH_CH = 16
TGRID = 16
LN_EPS = 0.01
BETA_ONE = 0.9
BETA_TWO = 0.99
ADAM_EPS = 1e-08

LANES = 128
PAD = 8
STEP = 16
UNROLL = 4
F32 = jnp.float32
BF16 = jnp.bfloat16
SLACK = 4 * 1024 * 1024


def position_tables(seq, width):
    half = width // 2
    freqs = np.exp(-math.log(10000.0) * np.arange(half, dtype=np.float64) / half)
    coarse = 8.0 * np.arange(seq // 8)[:, None] * freqs[None, :]
    fine = np.arange(8.0)[:, None] * freqs[None, :]
    return (
        np.stack([np.sin(coarse), np.cos(coarse)]).astype(np.float32),
        np.stack([np.sin(fine), np.cos(fine)]).astype(np.float32),
    )


def dot(a, b):
    return jnp.dot(a, b, preferred_element_type=F32)


def dot_t(a, b):
    return lax.dot_general(a, b, (((1,), (1,)), ((), ())), preferred_element_type=F32)


def dot_c(a, b):
    return lax.dot_general(a, b, (((0,), (0,)), ((), ())), preferred_element_type=F32)


def split3(x):
    one = x.astype(BF16).astype(F32)
    rest = x - one
    two = rest.astype(BF16).astype(F32)
    return (one, two, (rest - two).astype(BF16).astype(F32))


def left_parts(x):
    one, two, three = split3(x)
    return jnp.concatenate([one, one, one, two, two, three], axis=1).astype(BF16)


def right_parts(w):
    one, two, three = split3(w)
    return jnp.concatenate([one, two, three, one, two, one], axis=0).astype(BF16)


def unpack_tokens(packed):
    return jnp.concatenate(
        [packed[:, PATCH_CH * b : PATCH_CH * (b + 1)] for b in range(8)], axis=0
    )


def level(tau):
    lamb = 6.0 - 12.0 * (jnp.zeros((1, LANES), F32) + tau.astype(F32)) / TGRID
    alpha = jnp.sqrt(1.0 / (1.0 + jnp.exp(-lamb)))
    sigma = jnp.sqrt(1.0 / (1.0 + jnp.exp(lamb)))
    return (alpha, sigma)


def norm_rows(low, high, width):
    mean = (jnp.sum(low, 1, keepdims=True) + jnp.sum(high, 1, keepdims=True)) / width
    low = low - mean
    high = high - mean
    square = jnp.sum(low * low, 1, keepdims=True) + jnp.sum(high * high, 1, keepdims=True)
    inverse = lax.rsqrt(square / width + LN_EPS)
    return (low * inverse, high * inverse, inverse)


def position_rows(coarse, fine, start, seq):
    per = seq // 8
    b = start // per
    a = pl.multiple_of(start % per, STEP)
    sa = coarse[0, pl.ds(a, STEP), :]
    ca = coarse[1, pl.ds(a, STEP), :]
    sb = fine[0, pl.ds(b, 1), :]
    cb = fine[1, pl.ds(b, 1), :]
    return (sa * cb + ca * sb, ca * cb - sa * sb)


def centred(embed):
    return embed - jnp.mean(embed, axis=1, keepdims=True)


def square_rows(hid, pos, inv, count, width):
    W = width // 2

    def rows(i, _):
        at = pl.ds(pl.multiple_of(i * STEP, STEP), STEP)
        low = hid[at, 0:W] + pos[at, 0:W]
        high = hid[at, W:] + pos[at, W:]
        hid[at, 0:W] = low
        hid[at, W:] = high
        square = jnp.sum(low * low, 1, keepdims=True) + jnp.sum(high * high, 1, keepdims=True)
        inv[at, :] = jnp.broadcast_to(lax.rsqrt(square / width + LN_EPS), (STEP, LANES))
        return 0

    lax.fori_loop(0, count // STEP, rows, 0, unroll=UNROLL)


def shape_rows(hid, inv, scale_row, shift_row, shaped, count, width):
    def rows(i, _):
        at = pl.ds(pl.multiple_of(i * STEP, STEP), STEP)
        factor = inv[at, :]
        for c in range(width // LANES):
            lanes = slice(c * LANES, (c + 1) * LANES)
            shaped[at, lanes] = (
                hid[at, lanes] * factor * scale_row[:, lanes] + shift_row[:, lanes]
            ).astype(BF16)
        return 0

    lax.fori_loop(0, count // STEP, rows, 0, unroll=2)


def mod_row(table, which, index):
    return table[which, pl.ds(index, 1), :]


def head_masks(value):
    lane = lax.broadcasted_iota(jnp.int32, (1, LANES), 1)
    lower = (lane < HS).astype(F32)
    return (lower * value, (1.0 - lower) * value)


def probs_t(q, k, mask):
    scores = dot_t(k, q * mask.astype(BF16))
    expos = jnp.exp(scores - jnp.max(scores, axis=0, keepdims=True))
    return expos * (1.0 / jnp.sum(expos, axis=0, keepdims=True))


def attend_pair(q, k, v):
    small = head_masks(1.0 / math.sqrt(HS))
    one, two = (dot_c(v, probs_t(q, k, mask).astype(BF16)) for mask in small)
    return jnp.concatenate([one[0:HS], two[HS:]], axis=0).T.astype(BF16)


def quantize(x, ref, lead):
    top = jnp.maximum(jnp.max(jnp.abs(x), axis=0, keepdims=True), 1e-30)
    code = jnp.ceil(jnp.log(top) * (256.0 / math.log(2.0)))
    scale = jnp.exp(code * (math.log(2.0) / 256.0))
    rows = x.shape[0]
    ref[lead, 0:rows, :] = jnp.round(x * (32700.0 / scale)).astype(jnp.int32).astype(jnp.int16)
    ref[lead, rows : rows + PAD, :] = (
        jnp.broadcast_to(code, (PAD, x.shape[1])).astype(jnp.int32).astype(jnp.int16)
    )


def restore(ref, lead, rows):
    code = ref[lead, rows : rows + PAD, :].astype(jnp.int32).astype(F32)[0:1]
    scale = jnp.exp(code * (math.log(2.0) / 256.0)) * (1.0 / 32700.0)
    return ref[lead, 0:rows, :].astype(jnp.int32).astype(F32) * scale


VM = pl.BlockSpec(memory_space=pltpu.VMEM)
SM = pl.BlockSpec(memory_space=pltpu.SMEM)
ANY = pl.BlockSpec(memory_space=pl.ANY)
HB = pl.BlockSpec(memory_space=pltpu.HBM)


def stay(x):
    return (HB, pltpu.with_memory_space_constraint(x, pltpu.HBM))


def call(body, outs, ins, scratch, flops, after=()):
    out_shape = [jax.ShapeDtypeStruct(s, d) for s, d in outs]
    moved = sum(math.prod(s) * jnp.dtype(d).itemsize for s, d in outs)
    moved += sum(a.size * a.dtype.itemsize for _, a in ins)
    held = SLACK + moved
    held += sum(math.prod(a.shape) * jnp.dtype(a.dtype).itemsize for a in scratch if a.memory_space == pltpu.VMEM)
    held -= sum(a.size * a.dtype.itemsize for s, a in ins if s is ANY or s is HB)
    n, k = len(ins), len(after)

    def kernel(*refs):
        body(*refs[:n], *refs[n + k :])

    return pl.pallas_call(
        kernel,
        out_shape=out_shape,
        in_specs=[s for s, _ in ins] + [ANY] * k,
        out_specs=[VM] * len(outs),
        scratch_shapes=scratch,
        compiler_params=pltpu.CompilerParams(vmem_limit_bytes=int(held)),
        cost_estimate=pl.CostEstimate(
            flops=int(flops), bytes_accessed=int(moved), transcendentals=0
        ),
    )(*[a for _, a in ins], *after)


def all_sum(x, axis, n):
    return x + sum(shift(x, axis, n, s) for s in range(1, n))


def shift(x, axis, n, s):
    return lax.ppermute(x, axis, [(k, (k + s) % n) for k in range(n)])


def make_step(groups, peers, halves, dp):
    def inner_step(
        clean_latent,
        noise_draw,
        timestep,
        bucket,
        bucket_weights,
        teacher_embed,
        teacher_final,
        teacher_mod,
        teacher_qkv,
        teacher_out,
        student_embed,
        student_final,
        student_mod,
        student_qkv,
        student_out,
        moment_qkv,
        second_qkv,
        moment_out,
        second_out,
    ):
        G, R, M = groups, peers, halves
        width, inner = teacher_out.shape
        samples, latent = clean_latent.shape
        assert samples == 1
        seq = latent // PATCH_CH
        packed_rows = latent // LANES
        own = student_out.shape[0]
        half = seq // M
        W = width // 2
        cols = 3 * LANES
        z = lax.axis_index("dz")
        r = lax.axis_index("dr")
        m = lax.axis_index("mp")
        ids = jnp.concatenate(
            [timestep, bucket, jnp.stack([z, r, m]).astype(jnp.int32)]
        )
        coarse_np, fine_np = position_tables(seq, width)
        coarse = jnp.asarray(coarse_np)
        fine = jnp.asarray(fine_np)
        clean = clean_latent.reshape(packed_rows, LANES)
        noise = noise_draw.reshape(packed_rows, LANES)
        tmod = jnp.transpose(teacher_mod, (1, 0, 2))
        smod = jnp.transpose(student_mod, (1, 0, 2))
        tqkv = jnp.transpose(teacher_qkv, (1, 0, 2))
        sqkv = jnp.transpose(student_qkv, (1, 0, 2))
        chunk_rows = 3 * own
        extra = 3 * packed_rows + PAD

        def prologue(ids_ref, clean_h, noise_h, qkv_h, *refs):
            outs = refs[:G]
            clean_ref, noise_ref, qkv_ref, sems = refs[G:]
            loads = [
                pltpu.make_async_copy(qkv_h, qkv_ref, sems.at[0]),
                pltpu.make_async_copy(clean_h, clean_ref, sems.at[1]),
                pltpu.make_async_copy(noise_h, noise_ref, sems.at[2]),
            ]
            for c in loads:
                c.start()
            alpha, sigma = level(2 * ids_ref[0])
            for c in loads:
                c.wait()
            parts = split3(alpha * clean_ref[...] + sigma * noise_ref[...])
            mark = (jnp.zeros((PAD, LANES), F32) + ids_ref[0].astype(F32)).astype(BF16)
            for s in range(G):
                to = lax.rem(ids_ref[2] + s, G)
                lanes = pl.ds(pl.multiple_of(to * LANES, LANES), LANES)
                for t in range(3):
                    outs[s][t * own : (t + 1) * own, :] = qkv_ref[t, :, lanes]
                for j in range(3):
                    base = chunk_rows + j * packed_rows
                    outs[s][base : base + packed_rows, :] = parts[j].astype(BF16)
                outs[s][chunk_rows + 3 * packed_rows :, :] = mark

        pieces = call(
            prologue,
            [((chunk_rows + extra, LANES), BF16)] * G,
            [(SM, ids), stay(clean), stay(noise), stay(sqkv)],
            [
                pltpu.VMEM((packed_rows, LANES), F32),
                pltpu.VMEM((packed_rows, LANES), F32),
                pltpu.VMEM((3, own, inner), BF16),
                pltpu.SemaphoreType.DMA((3,)),
            ],
            1e6,
        )
        got = [pieces[0]] + [shift(pieces[s], "dz", G, s) for s in range(1, G)]
        bundle = jnp.stack([g[:chunk_rows] for g in got])
        bundles = [bundle] + [shift(bundle, "dr", R, s) for s in range(1, R)]

        def place(ids_ref, s, y):
            rr = lax.rem(ids_ref[3] + (R - s), R)
            zz = lax.rem(ids_ref[2] + (G - y), G)
            return pl.ds(pl.multiple_of((zz * R + rr) * own, own), own)

        def spread(ids_ref, parts, target):
            for s in range(M):
                at = pl.multiple_of(lax.rem(ids_ref[4] + (M - s), M) * half, half)
                target[pl.ds(at, half), :] = parts[s][...]

        def teacher_body(ids_ref, index, lat, embed, mod, pos, w_v, o_v, outs, tmp, waits):
            hid, inv, shaped, qkv_s, att = tmp
            hid[...] = dot(left_parts(lat), right_parts(centred(embed[...])))
            square_rows(hid, pos, inv, seq, width)
            shape_rows(
                hid, inv, 1.0 + mod_row(mod, 1, index), mod_row(mod, 0, index), shaped, seq, width
            )
            for t in range(3):
                waits[t]()
                qkv_s[t] = dot(shaped[...], w_v[t]).astype(BF16)
            for p in range(inner // LANES):
                lanes = slice(p * LANES, (p + 1) * LANES)
                att[:, lanes] = attend_pair(
                    qkv_s[0, :, lanes], qkv_s[1, :, lanes], qkv_s[2, :, lanes]
                )
            waits[3]()
            for s in range(1, M):
                at = pl.multiple_of(lax.rem(ids_ref[4] + s, M) * half, half)
                outs[s][...] = dot_t(att[pl.ds(at, half), :], o_v[...])
            mine = pl.multiple_of(ids_ref[4] * half, half)
            outs[0][...] = hid[pl.ds(mine, half), :] + mod_row(mod, 2, index) * dot_t(
                att[pl.ds(mine, half), :], o_v[...]
            )

        teacher_tmp = [
            pltpu.VMEM((seq, width), F32),
            pltpu.VMEM((seq, LANES), F32),
            pltpu.VMEM((seq, width), BF16),
            pltpu.VMEM((3, seq, inner), BF16),
            pltpu.VMEM((seq, inner), BF16),
        ]
        T = len(teacher_tmp)

        def teacher_front_first():
            def body(ids_ref, *refs):
                hbm = refs[:9]
                outs = refs[9 : 9 + M]
                lat_o, pos, w_v, o_v, piece = refs[9 + M : 14 + M]
                tmp = refs[14 + M : 14 + M + T]
                clean_v, noise_v, embed, mod, coarse_r, fine_r, sems = refs[14 + M + T :]
                targets = [clean_v, noise_v, embed, mod, coarse_r, fine_r]
                loads = [
                    pltpu.make_async_copy(hbm[j], targets[j], sems.at[j]) for j in range(6)
                ]
                big = [
                    pltpu.make_async_copy(hbm[6].at[t], w_v.at[t], sems.at[6 + t])
                    for t in range(3)
                ]
                big.append(pltpu.make_async_copy(hbm[7], o_v, sems.at[9]))
                aside = pltpu.make_async_copy(hbm[8], piece, sems.at[10])
                for c in loads + big + [aside]:
                    c.start()
                alpha, sigma = level(2 * ids_ref[0])
                for c in loads:
                    c.wait()

                def rows(i, _):
                    start = pl.multiple_of(i * STEP, STEP)
                    sin, cos = position_rows(coarse_r, fine_r, start, seq)
                    mean = (
                        jnp.sum(sin, 1, keepdims=True) + jnp.sum(cos, 1, keepdims=True)
                    ) / width
                    pos[pl.ds(start, STEP), 0:W] = sin - mean
                    pos[pl.ds(start, STEP), W:] = cos - mean
                    return 0

                lax.fori_loop(0, seq // STEP, rows, 0, unroll=2)
                lat = unpack_tokens(alpha * clean_v[...] + sigma * noise_v[...])
                lat_o[...] = lat
                teacher_body(
                    ids_ref,
                    2 * ids_ref[0] - 1,
                    lat,
                    embed,
                    mod,
                    pos,
                    w_v,
                    o_v,
                    outs,
                    tmp,
                    [c.wait for c in big],
                )
                aside.wait()

            params = [clean, noise, teacher_embed, tmod, coarse, fine, tqkv, teacher_out]
            params.append(student_out)
            return call(
                body,
                [((half, width), F32)] * M
                + [
                    ((seq, PATCH_CH), F32),
                    ((seq, width), F32),
                    ((3, width, inner), BF16),
                    ((width, inner), BF16),
                    ((own, inner), BF16),
                ],
                [(SM, ids)] + [stay(a) for a in params],
                teacher_tmp
                + [pltpu.VMEM(a.shape, a.dtype) for a in params[:6]]
                + [pltpu.SemaphoreType.DMA((11,))],
                2 * seq * width * inner * 4,
            )

        def teacher_front_second(lat_parts, pos, w_keep, o_keep):
            def body(ids_ref, embed, mod, pos_r, w_v, o_v, *refs):
                outs = refs[M : 2 * M]
                tmp = refs[2 * M : 2 * M + T]
                (lat_v,) = refs[2 * M + T :]
                spread(ids_ref, refs[:M], lat_v)
                teacher_body(
                    ids_ref,
                    2 * ids_ref[0] - 2,
                    lat_v[...],
                    embed,
                    mod,
                    pos_r,
                    w_v,
                    o_v,
                    outs,
                    tmp,
                    [lambda: None] * 4,
                )

            return call(
                body,
                [((half, width), F32)] * M,
                [
                    (SM, ids),
                    (VM, teacher_embed),
                    (VM, tmod),
                    (VM, pos),
                    (VM, w_keep),
                    (VM, o_keep),
                ]
                + [(VM, a) for a in lat_parts],
                teacher_tmp + [pltpu.VMEM((seq, PATCH_CH), F32)],
                2 * seq * width * inner * 4,
            )

        def tail_rows(mixed_refs, gate_row, parts_ref, norm_ref, inv_ref):
            def rows(i, _):
                start = pl.multiple_of(i * STEP, STEP)
                more_low = mixed_refs[1][pl.ds(start, STEP), 0:W]
                more_high = mixed_refs[1][pl.ds(start, STEP), W:]
                for ref in mixed_refs[2:]:
                    more_low = more_low + ref[pl.ds(start, STEP), 0:W]
                    more_high = more_high + ref[pl.ds(start, STEP), W:]
                low = mixed_refs[0][pl.ds(start, STEP), 0:W] + gate_row[:, 0:W] * more_low
                high = mixed_refs[0][pl.ds(start, STEP), W:] + gate_row[:, W:] * more_high
                low, high, inverse = norm_rows(low, high, width)
                if norm_ref is not None:
                    norm_ref[pl.ds(start, STEP), 0:W] = low
                    norm_ref[pl.ds(start, STEP), W:] = high
                    inv_ref[pl.ds(start, STEP), :] = jnp.broadcast_to(inverse, (STEP, LANES))
                for j, (a, b) in enumerate(zip(split3(low), split3(high))):
                    parts_ref[j, pl.ds(start, STEP), 0:W] = a.astype(BF16)
                    parts_ref[j, pl.ds(start, STEP), W:] = b.astype(BF16)
                return 0

            lax.fori_loop(0, half // STEP, rows, 0, unroll=UNROLL)

        def project(parts_ref, final_ref):
            f = jnp.concatenate(split3(final_ref[...]), axis=0).astype(BF16)
            C = PATCH_CH
            a = dot_t(parts_ref[0], f)
            b = dot_t(parts_ref[1], f)
            c = dot_t(parts_ref[2], f)
            tiny = a[:, 2 * C : 3 * C] + b[:, C : 2 * C] + c[:, 0:C]
            return (tiny + (a[:, C : 2 * C] + b[:, 0:C])) + a[:, 0:C]

        def narrow(pair):
            return tuple(x[:, 0:PATCH_CH] for x in pair)

        def teacher_tail(is_first, mixed, lat0, lat1=None, after=()):
            def body(ids_ref, *refs):
                mixed_refs = refs[:M]
                mod, final, lat_ref = refs[M : M + 3]
                out, parts = refs[-2:]
                first = 2 * ids_ref[0]
                index = first - 1 if is_first else first - 2
                tail_rows(mixed_refs, mod_row(mod, 2, index), parts, None, None)
                eps = project(parts, final)
                mine = pl.multiple_of(ids_ref[4] * half, half)
                latent0 = lat_ref[pl.ds(mine, half), :]
                af, sf = narrow(level(first))
                am, sm = narrow(level(first - 1))
                if is_first:
                    out[...] = am * (latent0 - sf * eps) / af + sm * eps
                else:
                    al, sl = narrow(level(first - 2))
                    latent2 = al * (refs[M + 3][...] - sm * eps) / am + sl * eps
                    out[...] = (latent0 - af / al * latent2) / (sf - af * sl / al)

            return call(
                body,
                [((half, PATCH_CH), F32)],
                [(SM, ids)]
                + [(VM, a) for a in mixed]
                + [(VM, tmod), (VM, teacher_final), (VM, lat0)]
                + ([] if is_first else [(VM, lat1)]),
                [pltpu.VMEM((3, half, width), BF16)],
                1e9,
                after,
            )[0]

        def student_front(pos, after):
            def body(ids_ref, embed, mod, pos_r, *refs):
                bun = refs[:R]
                lats = refs[R : R + G]
                atts = refs[R + G : R + 2 * G]
                qkv_o, shaped_o = refs[R + 2 * G : R + 2 * G + 2]
                w_v, hid, inv, lat_v, att_v, mod_v, right = refs[R + 2 * G + 2 :]
                for s in range(R):
                    for y in range(G):
                        at = place(ids_ref, s, y)
                        for t in range(3):
                            w_v[at, t * LANES : (t + 1) * LANES] = bun[s][
                                y, t * own : (t + 1) * own, :
                            ]
                right[...] = right_parts(centred(embed[...]))
                for y in range(G):
                    lat_v[y] = lats[y][chunk_rows : chunk_rows + 3 * packed_rows, :]
                    step_of = lats[y][chunk_rows + 3 * packed_rows :, :].astype(F32)
                    shift_row = jnp.zeros((1, width), F32)
                    scale_row = jnp.zeros((1, width), F32)
                    for k in range(mod.shape[1]):
                        hit = step_of[0:1, 0:1] == float(k + 1)
                        shift_row = jnp.where(hit, mod[0, k : k + 1, :], shift_row)
                        scale_row = jnp.where(hit, mod[1, k : k + 1, :], scale_row)
                    mod_v[y, 0:1, :] = shift_row
                    mod_v[y, 1:2, :] = 1.0 + scale_row

                def image(y, _):
                    one, two, three = (
                        unpack_tokens(
                            lat_v[y, j * packed_rows : (j + 1) * packed_rows, :].astype(F32)
                        )
                        for j in range(3)
                    )
                    left = jnp.concatenate([one, one, one, two, two, three], axis=1)
                    hid[...] = dot(left.astype(BF16), right[...])
                    square_rows(hid, pos_r, inv, seq, width)
                    target = shaped_o.at[y]
                    shape_rows(
                        hid, inv, mod_v[y, 1:2, :], mod_v[y, 0:1, :], target, seq, width
                    )
                    qkv_o[y] = dot(target[...], w_v[...]).astype(BF16)
                    att_v[y] = attend_pair(
                        qkv_o[y, :, 0:LANES],
                        qkv_o[y, :, LANES : 2 * LANES],
                        qkv_o[y, :, 2 * LANES :],
                    )
                    return 0

                lax.fori_loop(0, G, image, 0)
                for y in range(G):
                    atts[y][...] = att_v[y]

            return call(
                body,
                [((seq, LANES), BF16)] * G
                + [
                    ((G, seq, cols), BF16),
                    ((G, seq, width), BF16),
                ],
                [(SM, ids), (VM, student_embed), (VM, smod), (VM, pos)]
                + [(VM, b) for b in bundles]
                + [(VM, a) for a in got],
                [
                    pltpu.VMEM((width, cols), BF16),
                    pltpu.VMEM((seq, width), F32),
                    pltpu.VMEM((seq, LANES), F32),
                    pltpu.VMEM((G, 3 * packed_rows, LANES), BF16),
                    pltpu.VMEM((G, seq, LANES), BF16),
                    pltpu.VMEM((G, 2, width), F32),
                    pltpu.VMEM((6 * PATCH_CH, width), BF16),
                ],
                2 * G * seq * width * cols,
                after,
            )

        def student_out_proj(att_pieces, lat0, pos, out_bundles):
            def body(ids_ref, embed, mod, pos_r, lat_ref, *refs):
                pieces_r = refs[:G]
                bun = refs[G : G + R]
                refs = refs[G + R :]
                outs = refs[:M]
                att_o, out_w, hid = refs[M:]
                for s in range(R):
                    for y in range(G):
                        out_w[place(ids_ref, s, y), :] = bun[s][y]
                for s in range(G):
                    at = pl.multiple_of(lax.rem(ids_ref[2] + s, G) * LANES, LANES)
                    att_o[:, pl.ds(at, LANES)] = pieces_r[s][...]
                for s in range(1, M):
                    at = pl.multiple_of(lax.rem(ids_ref[4] + s, M) * half, half)
                    outs[s][...] = dot_t(att_o[pl.ds(at, half), :], out_w[...])
                mine = pl.multiple_of(ids_ref[4] * half, half)
                hid[...] = dot_t(att_o[pl.ds(mine, half), :], out_w[...])
                outs[0][...] = dot(
                    left_parts(lat_ref[pl.ds(mine, half), :]), right_parts(centred(embed[...]))
                )
                gate_row = mod_row(mod, 2, ids_ref[0] - 1)

                def rows(i, _):
                    start = pl.multiple_of(i * STEP, STEP)
                    at = pl.ds(start, STEP)
                    there = pl.ds(pl.multiple_of(mine + start, STEP), STEP)
                    outs[0][at, :] = (
                        outs[0][at, :] + pos_r[there, :] + gate_row * hid[at, :]
                    )
                    return 0

                lax.fori_loop(0, half // STEP, rows, 0, unroll=UNROLL)

            return call(
                body,
                [((half, width), F32)] * M + [((seq, inner), BF16), ((width, inner), BF16)],
                [
                    (SM, ids),
                    (VM, student_embed),
                    (VM, smod),
                    (VM, pos),
                    (VM, lat0),
                ]
                + [(VM, a) for a in att_pieces]
                + [(VM, a) for a in out_bundles],
                [pltpu.VMEM((half, width), F32)],
                2 * seq * width * inner,
            )

        def last_tail(student_mixed, goal):
            def body(ids_ref, bw_ref, *refs):
                s_refs = refs[:M]
                sm_table, sf_w, goal_r, dproj, loss = refs[M : M + 5]
                parts, normed, inv, grad = refs[M + 5 :]
                target = goal_r[...]
                gate_row = mod_row(sm_table, 2, ids_ref[0] - 1)
                tail_rows(s_refs, gate_row, parts, normed, inv)
                error = project(parts, sf_w) - target
                weight = bw_ref[ids_ref[1]]
                loss[...] = jnp.broadcast_to(
                    weight * jnp.sum(jnp.sum(error * error, 1, keepdims=True), 0, keepdims=True),
                    (8, LANES),
                )
                grad[...] = dot(left_parts(2.0 * weight * error), right_parts(sf_w[...]))

                def rows(i, _):
                    start = pl.multiple_of(i * STEP, STEP)
                    at = pl.ds(start, STEP)
                    ul, uh = grad[at, 0:W], grad[at, W:]
                    nl, nh = normed[at, 0:W], normed[at, W:]
                    one = (jnp.sum(ul, 1, keepdims=True) + jnp.sum(uh, 1, keepdims=True)) / width
                    two = (
                        jnp.sum(ul * nl, 1, keepdims=True) + jnp.sum(uh * nh, 1, keepdims=True)
                    ) / width
                    inverse = inv[at, 0:1]
                    dproj[at, 0:W] = (
                        gate_row[:, 0:W] * ((ul - one - nl * two) * inverse)
                    ).astype(BF16)
                    dproj[at, W:] = (
                        gate_row[:, W:] * ((uh - one - nh * two) * inverse)
                    ).astype(BF16)
                    return 0

                lax.fori_loop(0, half // STEP, rows, 0, unroll=UNROLL)

            return call(
                body,
                [((half, width), BF16), ((8, LANES), F32)],
                [(SM, ids), (SM, bucket_weights)]
                + [(VM, a) for a in student_mixed]
                + [(VM, smod), (VM, student_final), (VM, goal)],
                [
                    pltpu.VMEM((3, half, width), BF16),
                    pltpu.VMEM((half, width), F32),
                    pltpu.VMEM((half, LANES), F32),
                    pltpu.VMEM((half, width), F32),
                ],
                3e9,
            )

        def back_out(d_proj, out_full):
            def body(ids_ref, out_w, *refs):
                outs = refs[M : M + G]
                (full,) = refs[M + G :]
                for s in range(M):
                    at = pl.multiple_of(lax.rem(ids_ref[4] + (M - s), M) * half, half)
                    full[pl.ds(at, half), :] = dot(refs[s][...], out_w[...]).astype(BF16)
                for s in range(G):
                    at = pl.multiple_of(lax.rem(ids_ref[2] + s, G) * LANES, LANES)
                    outs[s][...] = full[:, pl.ds(at, LANES)]

            return call(
                body,
                [((seq, LANES), BF16)] * G,
                [(SM, ids), (VM, out_full)] + [(VM, a) for a in d_proj],
                [pltpu.VMEM((seq, inner), BF16)],
                2 * seq * width * inner,
            )

        def emit(ids_ref, full, outs):
            for s in range(R):
                rr = lax.rem(ids_ref[3] + s, R)
                for y in range(G):
                    at = pl.multiple_of((y * R + rr) * own, own)
                    block = full[pl.ds(at, own), :]
                    if s == 0:
                        outs[0][y] = block
                    else:
                        quantize(block, outs[s], y)

        def payloads(n):
            return [((G, own, n), F32)] + [((G, own + PAD, n), jnp.int16)] * (R - 1)

        def grad_out_kernel(d_proj, attended, after):
            def body(ids_ref, att_ref, *refs):
                outs = refs[M : M + R]
                full, both = refs[M + R :]
                spread(ids_ref, refs[:M], both)
                full[...] = dot_c(both[...], att_ref[...])
                emit(ids_ref, full, outs)

            return call(
                body,
                payloads(inner),
                [(SM, ids), (VM, attended)] + [(VM, a) for a in d_proj],
                [pltpu.VMEM((width, inner), F32), pltpu.VMEM((seq, width), BF16)],
                2 * seq * width * inner,
                after,
            )

        def back_attention(d_atts, packed, shaped):
            def body(ids_ref, qkv_r, shaped_r, *refs):
                da = refs[:G]
                outs = refs[G : G + R]
                full, pack, da_v = refs[G + R :]
                for y in range(G):
                    da_v[y] = da[y][...]
                small = head_masks(1.0 / math.sqrt(HS))
                plain = head_masks(1.0)

                def image(y, _):
                    q = qkv_r[y, :, 0:LANES]
                    k = qkv_r[y, :, LANES : 2 * LANES]
                    v = qkv_r[y, :, 2 * LANES :]
                    d_att = da_v[y]
                    d_query = []
                    d_key = None
                    d_value = None
                    for h in range(2):
                        w = probs_t(q, k, small[h])
                        d_prob = dot_t(v, d_att * small[h].astype(BF16))
                        inside = jnp.sum(w * d_prob, axis=0, keepdims=True)
                        d_score = (w * (d_prob - inside)).astype(BF16)
                        d_query.append(dot_c(k, d_score)[h * HS : (h + 1) * HS])
                        key_part = dot(d_score, q) * plain[h]
                        value_part = dot(w.astype(BF16), d_att) * plain[h]
                        d_key = key_part if h == 0 else d_key + key_part
                        d_value = value_part if h == 0 else d_value + value_part
                    pack[:, 0:LANES] = jnp.concatenate(d_query, axis=0).T.astype(BF16)
                    pack[:, LANES : 2 * LANES] = d_key.astype(BF16)
                    pack[:, 2 * LANES :] = d_value.astype(BF16)
                    part = dot_c(shaped_r[y], pack[...])

                    @pl.when(y == 0)
                    def _():
                        full[...] = part

                    @pl.when(y > 0)
                    def _():
                        full[...] += part

                    return 0

                lax.fori_loop(0, G, image, 0)
                emit(ids_ref, full, outs)

            return call(
                body,
                payloads(cols),
                [(SM, ids), (VM, packed), (VM, shaped)] + [(VM, a) for a in d_atts],
                [
                    pltpu.VMEM((width, cols), F32),
                    pltpu.VMEM((seq, cols), BF16),
                    pltpu.VMEM((G, seq, LANES), BF16),
                ],
                2 * G * seq * width * cols,
            )

        def fold(own_r, others, full):
            acc = None
            for y in range(G):
                x = own_r[y]
                for ref in others:
                    x = x + restore(ref, y, own)
                full[y] = x
                part = jnp.sum(x * x, axis=0, keepdims=True)
                acc = part if acc is None else acc + part
            return jnp.sum(acc, 1, keepdims=True)

        def hand_on(ids_ref, full, outs):
            for s in range(G):
                block = full[lax.rem(ids_ref[2] + s, G)]
                if s == 0:
                    outs[0][...] = block
                else:
                    quantize(block, outs[s], 0)

        def passed(n):
            return [((own, n), F32)] + [((1, own + PAD, n), jnp.int16)] * (G - 1)

        def out_sum(mine, received):
            def body(ids_ref, *refs):
                outs = refs[R : R + G]
                full = refs[-1]
                fold(refs[0], refs[1:R], full)
                hand_on(ids_ref, full, outs)

            return call(
                body,
                passed(inner),
                [(SM, ids), (VM, mine)] + [(VM, a) for a in received],
                [pltpu.VMEM((G, own, inner), F32)],
                1e8,
            )

        def last_sum(mine, received, out_parts, loss_part):
            def body(ids_ref, loss_r, *refs):
                o_parts = refs[:G]
                refs = refs[G:]
                outs = refs[R : R + G]
                grad_o, total, full = refs[R + G :]
                squares = fold(refs[0], refs[1:R], full)
                hand_on(ids_ref, full, outs)
                x = o_parts[0][...]
                for ref in o_parts[1:]:
                    x = x + restore(ref, 0, own)
                grad_o[...] = x
                more = jnp.sum(jnp.sum(x * x, axis=0, keepdims=True), 1, keepdims=True)
                total[0:8, :] = jnp.broadcast_to(squares + more, (8, LANES))
                total[8:16, :] = loss_r[...]

            return call(
                body,
                passed(cols) + [((own, inner), F32), ((16, LANES), F32)],
                [(SM, ids), (VM, loss_part)]
                + [(VM, a) for a in out_parts]
                + [(VM, mine)]
                + [(VM, a) for a in received],
                [pltpu.VMEM((G, own, cols), F32)],
                1e8,
            )

        def adam_kernel(total, qkv_parts, grad_out, state):
            def body(ids_ref, total_r, *refs):
                parts = refs[:G]
                go, mq, vq, mo, vo = refs[G : G + 5]
                nmq, nvq, uq, nmo, nvo, uo = refs[G + 5 : G + 11]
                (grad,) = refs[G + 11 :]
                rms = jnp.sqrt(total_r[0:1, 0:1] / (4 * width * inner * M))
                factor = 1.0 / jnp.maximum(rms, 1.0)
                for s in range(G):
                    at = pl.multiple_of(lax.rem(ids_ref[2] + (G - s), G) * LANES, LANES)
                    block = parts[s][...] if s == 0 else restore(parts[s], 0, own)
                    for t in range(3):
                        grad[t, :, pl.ds(at, LANES)] = block[:, t * LANES : (t + 1) * LANES]

                def adam(g, moment, second):
                    g = g * factor
                    moment = BETA_ONE * moment + (1.0 - BETA_ONE) * g
                    second = BETA_TWO * second + (1.0 - BETA_TWO) * g * g
                    return (moment, second, moment / (jnp.sqrt(second) + ADAM_EPS))

                for t in range(3):
                    nmq[t], nvq[t], uq[t] = adam(grad[t], mq[t], vq[t])
                nmo[...], nvo[...], uo[...] = adam(go[...], mo[...], vo[...])

            return call(
                body,
                [((3, own, inner), F32)] * 3 + [((own, inner), F32)] * 3,
                [(SM, ids), (VM, total)]
                + [(VM, a) for a in qkv_parts]
                + [(VM, grad_out)]
                + [(VM, a) for a in state],
                [pltpu.VMEM((3, own, inner), F32)],
                1e8,
            )

        def exchange(outs):
            return [outs[0]] + [shift(outs[s], "mp", M, s) for s in range(1, M)]

        def whole(part):
            return [part] + [shift(part, "mp", M, s) for s in range(1, M)]

        def send(parts, axis, n, sign=1):
            return [shift(parts[s], axis, n, sign * s) for s in range(1, n)]

        *mixed_a, lat0, pos, w_keep, o_keep, out_piece = teacher_front_first()
        mixed_a = exchange(mixed_a)
        next_mine = teacher_tail(True, mixed_a, lat0)
        out_got = [out_piece] + send([out_piece] * G, "dz", G)
        out_bundle = jnp.stack(out_got)
        out_bundles = [out_bundle] + send([out_bundle] * R, "dr", R)
        mixed_b = teacher_front_second(whole(next_mine), pos, w_keep, o_keep)
        *att_out, packed, shaped = student_front(pos, (mixed_b[0],))
        mixed_b = exchange(mixed_b)
        att_pieces = [att_out[0]] + send(att_out, "dz", G, -1)
        goal = teacher_tail(False, mixed_b, lat0, next_mine, (att_out[0],))
        *mixed_s, attended, out_full = student_out_proj(att_pieces, lat0, pos, out_bundles)
        mixed_s = exchange(mixed_s)
        d_proj_mine, loss_part = last_tail(mixed_s, goal)
        d_proj = whole(d_proj_mine)
        d_out = back_out(d_proj, out_full)
        d_atts = [d_out[0]] + send(d_out, "dz", G)
        go = grad_out_kernel(d_proj, attended, (d_out[0],))
        go_recv = send(go, "dr", R)
        gq = back_attention(d_atts, packed, shaped)
        gq_recv = send(gq, "dr", R)
        go_z = out_sum(go[0], go_recv)
        out_parts = [go_z[0]] + send(go_z, "dz", G)
        *gq_z, grad_out, both = last_sum(gq[0], gq_recv, out_parts, loss_part)
        qkv_parts = [gq_z[0]] + send(gq_z, "dz", G)
        for axis, n in (("mp", M), ("dr", R), ("dz", G)):
            both = all_sum(both, axis, n)
        view = lambda a: jnp.transpose(a, (1, 0, 2))
        nmq, nvq, uq, nmo, nvo, uo = adam_kernel(
            both,
            qkv_parts,
            grad_out,
            [view(moment_qkv), view(second_qkv), moment_out, second_out],
        )
        loss = both[8, 0] / (samples * dp * latent)
        return (view(nmq), view(nvq), view(uq), nmo, nvo, uo, loss)

    return inner_step


def solution(mesh):
    dp, halves = mesh.shape["dp"], mesh.shape["mp"]

    def run(*args):
        groups = args[9].shape[1] // halves // LANES
        peers = dp // groups
        fine = Mesh(mesh.devices.reshape(groups, peers, halves), ("dz", "dr", "mp"))
        dd = ("dz", "dr")
        specs = (
            P(dd, None),
            P(dd, None),
            P(dd),
            P(dd),
            P(),
            P(),
            P(),
            P(),
            P(None, None, "mp"),
            P(None, "mp"),
            P(),
            P(),
            P(),
            P(dd, None, "mp"),
            P(dd, "mp"),
            P(dd, None, "mp"),
            P(dd, None, "mp"),
            P(dd, "mp"),
            P(dd, "mp"),
        )
        return jax.shard_map(
            make_step(groups, peers, halves, dp),
            mesh=fine,
            in_specs=specs,
            out_specs=(
                P(dd, None, "mp"),
                P(dd, None, "mp"),
                P(dd, None, "mp"),
                P(dd, "mp"),
                P(dd, "mp"),
                P(dd, "mp"),
                P(),
            ),
            check_vma=False,
        )(*args)

    return run
```
